32 devices in a mesh: gx: 8 (over y, x, core), gy: 4 (over z).
Axes of the slice: x: 2, y: 2, z: 4, core: 2. Of those that a mesh axis runs over, the one named last changes fastest.
Arguments:
- probes: float32 [16, 128, 128, 256], P(None, 'gx', 'gy'), may hold values from -6 to 6
- diffusivity: float32 [128, 128, 256], P('gx', 'gy'), may hold values from 0.5 to 2
- wind_speed: float32 [3], replicated, may hold values from 0.5 to 2
- sensor_cell: int32 [8, 4, 128], P('gx', 'gy'), may hold values from 0 to 131071
- sensor_owner: int32 [8, 4, 128, 1], P('gx', 'gy'), may hold values from 0 to 31; in each aligned block of 128 rows (0 to 127, 128 to 255, ..., all dimensions but the last counted through in order) at most 4 rows name the same one
- sensor_count: int32 [8, 4], P('gx', 'gy'), may hold values from 64 to 128
- goal_weight: float32 [8, 4, 128, 16], P('gx', 'gy'), may hold values from -0.6 to 0.6
Outputs:
- fields: float32 [16, 128, 128, 256], P(None, 'gx', 'gy')
- goal_block: float32 [512, 16], P(('gx', 'gy'))
- ritz_gram: float32 [16, 16], replicated
The draws below stay inside these ranges and needn't reach their ends.
Inputs may be any that keep to these rules, and one draw needn't show every extreme that they name: `sensor_owner`: among the rows of one device, no owner is named more than 4 times, a bound that some block reaches.
All inputs are finite; a program needn't handle non-finite values.
Results may differ from the reference program's by a relative error of at most 0.0003.
Values sent between devices are 32-bit elements; how exact they have to be, the bound alone decides.
A program may use at most 192 MiB of HBM per device.

```python
import math
import jax
import jax.numpy as jnp
import numpy as np
from jax import lax

CX = 16
CY = 32
CZ = 256
PROBES = 16
STEPS = 2
SWEEPS = 4
SENS = 128
CAP = 4
GOAL_DEV = 16
NX = 128
NY = 128
N_GX = 8
N_GY = 4


def place_ends(result, own_key, low, high):
    longest = result.shape.index(max(result.shape))
    spots = []
    for shift in (0, 1):
        where = [jax.random.randint(jax.random.fold_in(own_key, axis), (), 0, length) for axis, length in enumerate(result.shape)]
        where[longest] = (where[longest] + shift) % result.shape[longest]
        spots.append(tuple(where))
    return result.at[spots[0]].set(low).at[spots[1]].set(high)


def level_of(own_key, extent, cuts, least, high):
    def one(dim, parts):
        draws = jax.random.uniform(jax.random.fold_in(jax.random.fold_in(own_key, 6), dim), (parts,), jnp.float32, least / len(cuts), high / len(cuts))
        return jnp.repeat(jnp.exp(draws), extent[dim] // parts).reshape((-1,) + (1,) * (len(extent) - dim - 1))

    gain = one(*cuts[0])
    for cut in cuts[1:]:
        gain = gain * one(*cut)
    return gain


def shared_out(own_key, own, number, rows, count, top, bound, slope):
    ranking = jax.random.permutation(own_key, count)
    packed, common = shares(count, rows * top, bound, slope, True), shares(count, rows * top, bound, slope, False)
    places = jnp.arange(count)

    def named(lengths, turn):
        used = int((lengths > 0).sum())
        fixed = max(1, used // 4)
        shifted = fixed + (places - fixed + turn * (used - fixed)) % max(1, count - fixed)
        return jnp.zeros((count,), jnp.int32).at[ranking[jnp.where(places < fixed, places, shifted)]].set(jnp.asarray(lengths, jnp.int32))

    lengths = jnp.where(number % 4 == 0, named(packed, number // 4), named(common, number - number // 4 - 1))
    mixed = jax.random.permutation(jax.random.fold_in(own, 3), count)
    donor, sink = mixed[0:count // 2 * 2:2], mixed[1:count // 2 * 2:2]
    slack = jnp.minimum(lengths[donor] - 1, bound - lengths[sink]) // 2
    slack = jnp.where((donor == ranking[0]) | (sink == ranking[0]) | (lengths[sink] == 0), 0, jnp.maximum(slack, 0))
    shifted = jax.random.randint(jax.random.fold_in(own, 4), (count // 2,), 0, 1 << 20) % (slack + 1)
    lengths = lengths.at[donor].add(-shifted).at[sink].add(shifted)
    members = jnp.searchsorted(jnp.cumsum(lengths), jnp.arange(rows * top), side="right").astype(jnp.int32)
    table = members.reshape(top, rows).T
    table = table[jax.random.permutation(jax.random.fold_in(own, 1), rows)]
    turn = jax.random.randint(jax.random.fold_in(own, 2), (rows, 1), 0, top)
    return jnp.take_along_axis(table, (jnp.arange(top)[None, :] + turn) % top, axis=1)


def shares(number_of, total, limit, slope, full):
    weights = [(1 << 20) // math.isqrt(rank ** slope) + 1 for rank in range(1, number_of + 1)]
    largest = limit if full else min(limit, max(-(-total // number_of), total * weights[0] // sum(weights)))
    least = 1 if total - largest >= number_of - 1 else 0
    given, rest = [largest] + [least] * (number_of - 1), total - largest - least * (number_of - 1)
    while rest > 0:
        movable = [i for i in range(1, number_of) if given[i] < largest] or [i for i in range(1, number_of) if given[i] < limit]
        whole, left = sum([weights[i] for i in movable]), rest
        for i in movable:
            extra = min(limit - given[i], max(1, left * weights[i] // whole), rest)
            given[i] = given[i] + extra
            rest = rest - extra
    return np.array(given)


def centred(key, extent, spread, reach, cuts=(), held_as=jnp.bfloat16):
    level = level_of(key, extent, cuts, -0.22, 0.18) if cuts else 1.0
    entries = jax.random.normal(key, extent, jnp.float32) * spread * level
    return jnp.minimum(jnp.maximum(entries, -reach), reach).astype(held_as)


def setup_inputs(seed: int = 0) -> dict:
    arg_keys = jax.random.split(jax.random.key(seed), 8)
    probes = centred(arg_keys[0], (PROBES, NX, NY, CZ), 1.0, 6.0, ((1, 8), (2, 4)), jnp.float32)
    diffusivity = jnp.clip(jnp.exp(math.log(2.0) - 1.3862944 * jax.random.uniform(arg_keys[1], (NX, NY, CZ), jnp.float32) ** level_of(arg_keys[1], (NX, NY, CZ), ((0, 8), (1, 4)), -0.2, 0.2)), 0.5, 2.0)
    wind_speed = jnp.clip(jax.random.uniform(arg_keys[2], (3,), jnp.float32, 0.5, 2.0), 0.5, 2.0)
    sensor_cell = place_ends(jax.random.randint(arg_keys[3], (N_GX, N_GY, SENS), 0, CX * CY * CZ), jax.random.fold_in(arg_keys[3], 1), 0, (CX * CY * CZ) - 1).astype(jnp.int32)
    sensor_owner_keys = jax.random.split(jax.random.fold_in(arg_keys[4], 1), N_GX * N_GY * SENS // SENS)
    sensor_owner_turns = jax.random.permutation(jax.random.fold_in(arg_keys[4], 3), N_GX * N_GY * SENS // SENS)
    sensor_owner = jax.vmap(lambda own, number: shared_out(jax.random.fold_in(arg_keys[4], 2), own, number, SENS, N_GX * N_GY, 1, CAP, 1))(sensor_owner_keys, sensor_owner_turns).reshape((N_GX, N_GY, SENS, 1))
    sensor_count = place_ends(jax.random.randint(arg_keys[5], (N_GX, N_GY), SENS // 2, SENS + 1), jax.random.fold_in(arg_keys[5], 1), SENS // 2, SENS).astype(jnp.int32)
    goal_weight = centred(arg_keys[6], (N_GX, N_GY, SENS, GOAL_DEV), 0.1, 0.6, ((0, 8), (1, 4)), jnp.float32)
    return dict(probes=probes, diffusivity=diffusivity, wind_speed=wind_speed, sensor_cell=sensor_cell, sensor_owner=sensor_owner, sensor_count=sensor_count, goal_weight=goal_weight)


time_step = 2.0


def relax(padded, source, diffusion, wind_speed):
    centre = padded[..., 1:-1, 1:-1, :]
    widths = [(0, 0)] * (centre.ndim - 1) + [(1, 1)]
    zpadded = jnp.pad(centre, widths)
    beside = padded[..., 2:, 1:-1, :] + padded[..., :-2, 1:-1, :]
    beside = beside + padded[..., 1:-1, 2:, :] + padded[..., 1:-1, :-2, :]
    beside = beside + zpadded[..., 2:] + zpadded[..., :-2]
    upwind = wind_speed[0] * padded[..., :-2, 1:-1, :] + wind_speed[1] * padded[..., 1:-1, :-2, :] + wind_speed[2] * zpadded[..., :-2]
    diagonal = 1.0 + time_step * (6.0 * diffusion + wind_speed[0] + wind_speed[1] + wind_speed[2])
    updated = (source + time_step * (diffusion * beside + upwind)) / diagonal
    return jnp.where(diffusion > 0.0, updated, 0.0)


def reference(probes, diffusivity, wind_speed, sensor_cell, sensor_owner, sensor_count, goal_weight):
    def advance(state_field):
        for step_index in range(STEPS):
            source = state_field
            for sweep_index in range(SWEEPS):
                state_field = relax(jnp.pad(state_field, ((1, 1), (1, 1), (0, 0))), source, diffusivity, wind_speed)
        return state_field

    fields = lax.map(advance, probes)
    blocks = fields.reshape(PROBES, N_GX, CX, N_GY, CY, CZ).transpose(1, 3, 0, 2, 4, 5)
    blocks = blocks.reshape(N_GX, N_GY, PROBES, CX * CY * CZ)
    readings = jnp.take_along_axis(blocks, sensor_cell[:, :, None, :].astype(jnp.int32), axis=3)
    active = (jnp.arange(SENS, dtype=jnp.int32)[None, None, :] < sensor_count[:, :, None]).astype(jnp.float32)
    readings = readings.transpose(0, 1, 3, 2) * active[..., None]
    outer = (goal_weight[..., :, None] * readings[..., None, :]).reshape(N_GX * N_GY * SENS, GOAL_DEV * PROBES)
    owners = sensor_owner.reshape(-1)
    onehot = (owners[:, None] == jnp.arange(N_GX * N_GY, dtype=jnp.int32)[None, :]).astype(jnp.float32)
    goal_block = jnp.dot(onehot.T, outer, precision=lax.Precision.HIGHEST).reshape(N_GX * N_GY * GOAL_DEV, PROBES)
    ritz_gram = jnp.dot(goal_block.T, goal_block, precision=lax.Precision.HIGHEST)
    return fields, goal_block, ritz_gram
```

```python
import math

import jax
import jax.numpy as jnp
from jax import lax
from jax.experimental import pallas as pl
from jax.experimental.pallas import tpu as pltpu
from jax.sharding import PartitionSpec as P

STEPS = 2
SWEEPS = 4

time_step = 2.0

LANES = 8
CHUNK = 8
TILE = 128
MESH = pl.DeviceIdType.MESH


def buffers(k):
    read = 0 if k == 0 else 2 - k % 2
    written = 0 if k == SWEEPS - 1 else 1 + k % 2
    return read, 0, written


def chips_in_row(n_gx):
    row = math.isqrt(max(n_gx // 2, 0))
    return row if row >= 2 and 2 * row * row == n_gx else 0


def unflatten(flat, columns):
    per = TILE // columns
    sub = lax.broadcasted_iota(jnp.int32, (per, TILE), 0)
    lane = lax.broadcasted_iota(jnp.int32, (per, TILE), 1)
    tiles = []
    for t in range(flat.shape[0]):
        wide = jnp.broadcast_to(flat[t : t + 1], (per, TILE))
        rows = wide
        for j in range(1, per):
            rows = jnp.where(sub == j, pltpu.roll(wide, TILE - columns * j, 1), rows)
        tiles.append(jnp.where(lane < columns, rows, 0.0))
    return jnp.concatenate(tiles, axis=0)


def flatten(rows, columns):
    per = TILE // columns
    sub = lax.broadcasted_iota(jnp.int32, (per, TILE), 0)
    tiles = []
    for t in range(rows.shape[0] // per):
        part = rows[t * per : (t + 1) * per]
        flat = jnp.where(sub == 0, part, 0.0)
        for j in range(1, per):
            flat = flat + jnp.where(sub == j, pltpu.roll(part, columns * j, 1), 0.0)
        tiles.append(jnp.sum(flat, axis=0, keepdims=True))
    return jnp.concatenate(tiles, axis=0)


def whole_kernel(
    wind_in, cells_in, count_in, field, diffusivity, weights_in, owners_in,
    state, goal_out, gram_out,
    held0, held1, held2, inv, mix, passing, contrib, landed, gram_mine, gram_landed, wind, cells, count, weights, owners,
    load_sem, small_sem, send_sem, recv_sem, pass_recv, pass_send, term_sem, gram_sem,
):
    held = (held0, held1, held2)
    groups, nx, ny = held0.shape[0], held0.shape[1] - 2, held0.shape[2] - 2
    nz = held0.shape[4]
    tiles = nz // TILE
    half = ny // 2
    gx, gy = lax.axis_index("gx"), lax.axis_index("gy")
    n_gx, n_gy = lax.axis_size("gx"), lax.axis_size("gy")
    devices = n_gx * n_gy
    me = gx * n_gy + gy
    xs, ys = pl.ds(1, nx), pl.ds(1, ny)
    row = chips_in_row(n_gx)

    def place(k):
        other = lax.rem(me + k, devices)
        return (lax.div(other, n_gy), lax.rem(other, n_gy))

    barrier = pltpu.get_barrier_semaphore()

    def greet(k, carry):
        pl.semaphore_signal(barrier, inc=1, device_id=place(k), device_id_type=MESH)
        return carry

    lax.fori_loop(1, devices, greet, 0)

    small = [
        pltpu.make_async_copy(src, dst, small_sem.at[i])
        for i, (src, dst) in enumerate(
            ((wind_in, wind), (cells_in, cells), (count_in, count), (weights_in, weights), (owners_in, owners))
        )
    ]
    small[0].start()

    def load(part, p):
        where = (pl.ds(0, 1), pl.ds(nx - 1, 1), pl.ds(1, nx - 2))[part]
        land = (pl.ds(1, 1), pl.ds(nx, 1), pl.ds(2, nx - 2))[part]
        return pltpu.make_async_copy(
            field.at[p, where],
            held0.at[p // LANES, land, ys, p % LANES],
            load_sem.at[part, p],
        )

    probes = groups * LANES
    for p in range(probes):
        load(0, p).start()
        load(1, p).start()
    for p in range(LANES):
        load(2, p).start()
    coefficient = pltpu.make_async_copy(diffusivity, mix, load_sem.at[3, 0])
    coefficient.start()
    for p in range(LANES, probes):
        load(2, p).start()
    for copy in small[1:]:
        copy.start()

    has_up, has_down = gx < n_gx - 1, gx > 0
    has_next, has_back = gy < n_gy - 1, gy > 0
    blank_x = jnp.zeros((ny, LANES, nz), jnp.float32)
    blank_y = jnp.zeros((nx, LANES, nz), jnp.float32)

    @pl.when(jnp.logical_not(has_down))
    def _():
        for b in range(3):
            for g in range(groups):
                held[b][g, 0, ys] = blank_x

    @pl.when(jnp.logical_not(has_up))
    def _():
        for b in range(3):
            for g in range(groups):
                held[b][g, nx + 1, ys] = blank_x

    @pl.when(jnp.logical_not(has_back))
    def _():
        for b in range(3):
            for g in range(groups):
                held[b][g, xs, 0] = blank_y

    @pl.when(jnp.logical_not(has_next))
    def _():
        for b in range(3):
            for g in range(groups):
                held[b][g, xs, ny + 1] = blank_y

    pl.semaphore_wait(barrier, devices - 1)

    if row:
        wide = 2 * row
        far_up = jnp.logical_and(has_up, lax.rem(gx, wide) == wide - 1)
        far_down = jnp.logical_and(has_down, lax.rem(gx, wide) == 0)
        passes = (
            jnp.logical_and(gx >= wide, lax.rem(gx, wide) == wide - 1),
            jnp.logical_and(gx < n_gx - wide, lax.rem(gx, wide) == 0),
        )
        pass_from = ((gx + wide, gy), (gx - wide, gy))
        pass_to = ((gx - wide + 1, gy), (gx + wide - 1, gy))
        near_up = jnp.logical_and(has_up, lax.rem(gx, wide) != wide - 1)
        near_down = jnp.logical_and(has_down, lax.rem(gx, wide) != 0)
    else:
        near_up, near_down = has_up, has_down

    routes = ((gx + 1, gy), (gx - 1, gy), (gx, gy + 1), (gx, gy - 1))
    sends = (has_up, has_up, has_down, has_down, has_next, has_back)
    receives = (has_down, has_down, has_up, has_up, has_back, has_next)

    def face(d, b, g, turn):
        if d < 4:
            rows = pl.ds(1 + (d % 2) * half, half)
            if d < 2:
                src, dst, target = held[b].at[g, nx, rows], held[b].at[g, 0, rows], routes[0]
            else:
                src, dst, target = held[b].at[g, 1, rows], held[b].at[g, nx + 1, rows], routes[1]
        elif d == 4:
            src, dst, target = held[b].at[g, xs, ny], held[b].at[g, xs, 0], routes[2]
        else:
            src, dst, target = held[b].at[g, xs, 1], held[b].at[g, xs, ny + 1], routes[3]
        return pltpu.make_async_remote_copy(
            src_ref=src,
            dst_ref=dst,
            send_sem=send_sem.at[turn % 2, g, d],
            recv_sem=recv_sem.at[turn % 2, g, d],
            device_id=target,
            device_id_type=MESH,
        )

    def detour(way, b, g, turn):
        rows = pl.ds(1 + half, half)
        return pltpu.make_async_remote_copy(
            src_ref=held[b].at[g, (nx, 1)[way], rows],
            dst_ref=passing.at[turn, g],
            send_sem=send_sem.at[turn % 2, g, 2 * way + 1],
            recv_sem=pass_recv.at[turn, g],
            device_id=pass_from[way],
            device_id_type=MESH,
        )

    def onward(way, b, g, turn):
        rows = pl.ds(1 + half, half)
        return pltpu.make_async_remote_copy(
            src_ref=passing.at[turn, g],
            dst_ref=held[b].at[g, (0, nx + 1)[way], rows],
            send_sem=pass_send.at[turn, g],
            recv_sem=recv_sem.at[turn % 2, g, 2 * way + 1],
            device_id=pass_to[way],
            device_id_type=MESH,
        )

    def start(d, b, g, turn):
        @pl.when((near_up, near_down)[d // 2] if d in (1, 3) else sends[d])
        def _():
            face(d, b, g, turn).start()

        if row and d in (1, 3):
            @pl.when((far_up, far_down)[d // 2])
            def _():
                detour(d // 2, b, g, turn).start()

    def start_x(b, g, turn):
        for d in (1, 3, 0, 2):
            start(d, b, g, turn)

    def start_y(b, g, turn):
        for d in (4, 5):
            start(d, b, g, turn)

    def wait_sends(b, g, turn):
        for d in range(6):
            @pl.when(sends[d])
            def _():
                face(d, b, g, turn).wait_send()

    def wait_recv(ways, b, g, turn):
        for d in ways:
            @pl.when(receives[d])
            def _():
                face(d, b, g, turn).wait_recv()

    def pass_on(b, g, turn):
        if row:
            for way in (0, 1):
                @pl.when(passes[way])
                def _():
                    detour(way, b, g, turn).wait_recv()
                    onward(way, b, g, turn).start()

    def pass_done(b, g, turn):
        if row:
            for way in (0, 1):
                @pl.when(passes[way])
                def _():
                    onward(way, b, g, turn).wait_send()

    for g in range(groups):
        for p in range(g * LANES, (g + 1) * LANES):
            load(0, p).wait()
            load(1, p).wait()
        start_x(0, g, 0)

    small[0].wait()
    w0, w1, w2 = time_step * wind[0], time_step * wind[1], time_step * wind[2]
    total_wind = wind[0] + wind[1] + wind[2]

    def coefficients(x, carry):
        a = mix[x]
        r = 1.0 / (1.0 + time_step * (6.0 * a + total_wind))
        inv[x] = jnp.where(a > 0.0, r, 0.0)
        mix[x] = jnp.where(a > 0.0, time_step * a * r, 0.0)
        return carry

    for g in range(groups):
        for p in range(g * LANES, (g + 1) * LANES):
            load(2, p).wait()
        start_y(0, g, 0)
        if g == 0:
            coefficient.wait()
            lax.fori_loop(0, nx, coefficients, 0)
    for g in range(groups):
        pass_on(0, g, 0)

    lane = lax.broadcasted_iota(jnp.int32, (LANES, TILE), 1)
    first, last_lane = lane == 0, lane == TILE - 1
    zero = jnp.zeros((LANES, TILE), jnp.float32)

    def plane(x, g, read, source, put):
        def tile(b, x, y, t):
            return held[b][g, x, y, :, t * TILE : (t + 1) * TILE]

        low = [tile(read, x, 0, t) for t in range(tiles)]
        centre = [tile(read, x, 1, t) for t in range(tiles)]
        for y in range(1, ny + 1):
            i, k = divmod(y - 1, CHUNK)
            high = [tile(read, x, y + 1, t) for t in range(tiles)]
            down = [pltpu.roll(c, 1, 1) for c in centre]
            up = [pltpu.roll(c, TILE - 1, 1) for c in centre]
            for t in range(tiles):
                cols = slice(t * TILE, (t + 1) * TILE)
                z_low = lax.select(first, down[t - 1] if t else zero, down[t])
                z_high = lax.select(last_lane, up[t + 1] if t + 1 < tiles else zero, up[t])
                x_low = tile(read, x - 1, y, t)
                x_high = tile(read, x + 1, y, t)
                beside = (x_low + x_high) + (low[t] + high[t]) + (z_low + z_high)
                upwind = w0 * x_low + w1 * low[t] + w2 * z_low
                begun = tile(source, x, y, t)
                r = jnp.broadcast_to(inv[x - 1, i, k : k + 1, cols], (LANES, TILE))
                a = jnp.broadcast_to(mix[x - 1, i, k : k + 1, cols], (LANES, TILE))
                put(g, x, y, cols, (begun + upwind) * r + a * beside)
            low, centre = centre, high

    total = STEPS * SWEEPS

    def sweep(step, k, last=False):
        read, source, written = buffers(k)
        turn = step * SWEEPS + k
        if last:
            def put(g, x, y, cols, value):
                state[g, x - 1, y - 1, :, cols] = value
        else:
            def put(g, x, y, cols, value):
                held[written][g, x, y, :, cols] = value

        def group(g, carry):
            def end(i, carry):
                plane(1 + i * (nx - 1), g, read, source, put)
                return carry

            def inner(x, carry):
                plane(x, g, read, source, put)
                return carry

            @pl.when(turn >= 1)
            def _():
                wait_sends(read, g, turn - 1)

            wait_recv((4, 5), read, g, turn)
            if last:
                lax.fori_loop(2, nx, inner, 0)
            wait_recv((0, 1, 2, 3), read, g, turn)
            lax.fori_loop(0, 2, end, 0)
            if not last:
                start_x(written, g, turn + 1)
                lax.fori_loop(2, nx, inner, 0)
                start_y(written, g, turn + 1)
                pass_on(written, g, turn + 1)
            return carry

        lax.fori_loop(0, groups, group, 0)

    def one_step(step, carry):
        for k in range(SWEEPS - 1):
            sweep(step, k)

        @pl.when(step < STEPS - 1)
        def _():
            sweep(step, SWEEPS - 1)

        return carry

    lax.fori_loop(0, STEPS, one_step, 0)
    sweep(STEPS - 1, SWEEPS - 1, True)
    for g in range(groups):
        wait_sends(0, g, total - 1)
        lax.fori_loop(0, total, lambda turn, carry: pass_done(0, g, turn) or carry, 0)
    for copy in small[1:]:
        copy.wait()

    sensors = cells.shape[0]

    column_of = lax.broadcasted_iota(jnp.int32, (LANES, nz), 1)
    unroll = math.gcd(sensors, 32)

    def look(i, carry):
        acc = list(carry)
        for k in range(unroll):
            s = i * unroll + k
            cell = cells[s]
            column = lax.div(cell, nz)
            hit = column_of == lax.rem(cell, nz)
            for g in range(groups):
                value = lax.select(hit, state[g, lax.div(column, ny), lax.rem(column, ny)], jnp.zeros((LANES, nz), jnp.float32))
                acc[g] = jnp.where(lane == s, jnp.sum(value, axis=1, keepdims=True), acc[g])
        return tuple(acc)

    readings = jnp.concatenate(lax.fori_loop(0, sensors // unroll, look, (zero,) * groups), axis=0)
    active = lax.broadcasted_iota(jnp.int32, (probes, sensors), 1) < count[0]
    readings = jnp.where(active, readings, 0.0)
    weight = weights[...]
    goal_count = weight.shape[0]
    outer = (weight[:, None, :] * readings[None, :, :]).reshape(goal_count * probes, sensors)
    onehot = (
        lax.broadcasted_iota(jnp.int32, (devices, sensors), 0) == jnp.broadcast_to(owners[...], (devices, sensors))
    ).astype(jnp.float32)
    terms = lax.dot_general(
        onehot, outer, (((1,), (1,)), ((), ())),
        precision=lax.Precision.HIGHEST, preferred_element_type=jnp.float32,
    )
    spans = contrib.shape[1]
    for t in range(spans):
        contrib[:, t, :] = terms[:, t * TILE : (t + 1) * TILE]

    def exchange(source, into, sem):
        def copy(k, slot):
            return pltpu.make_async_remote_copy(
                src_ref=source(k),
                dst_ref=into.at[slot],
                send_sem=sem.at[0, k],
                recv_sem=sem.at[1, k],
                device_id=place(k),
                device_id_type=MESH,
            )

        def send(k, carry):
            copy(k, me).start()
            return carry

        def finish(k, carry):
            arriving = copy(k, lax.rem(me + devices - k, devices))
            arriving.wait_send()
            arriving.wait_recv()
            return carry

        lax.fori_loop(1, devices, send, 0)
        into[pl.ds(me, 1)] = source(0)[...][None]
        lax.fori_loop(1, devices, finish, 0)
        return jnp.sum(into[...], axis=0)

    goal = exchange(lambda k: contrib.at[lax.rem(me + k, devices)], landed, term_sem)
    goal = unflatten(goal, probes)
    goal_out[...] = goal[:, :probes]
    gram = jnp.dot(
        goal.T[:probes], goal, precision=lax.Precision.HIGHEST, preferred_element_type=jnp.float32
    )
    gram_mine[...] = flatten(gram, probes)
    gram = exchange(lambda k: gram_mine, gram_landed, gram_sem)
    gram_out[...] = unflatten(gram, probes)[:, :probes]


def store_kernel(state, goal, gram, out, goal_out, gram_out, store_sem, small_sem):
    copies = [
        pltpu.make_async_copy(state.at[p // LANES, :, :, p % LANES], out.at[p], store_sem.at[p])
        for p in range(out.shape[0])
    ]
    copies.append(pltpu.make_async_copy(goal, goal_out, small_sem.at[0]))
    copies.append(pltpu.make_async_copy(gram, gram_out, small_sem.at[1]))
    for copy in copies:
        copy.start()
    for copy in copies:
        copy.wait()


def body(probes, diffusivity, wind_speed, sensor_cell, sensor_owner, sensor_count, goal_weight):
    probe_count, nx, ny, nz = probes.shape
    groups = probe_count // LANES
    sensors, goal_count = sensor_cell.shape[2], goal_weight.shape[3]
    devices = lax.axis_size("gx") * lax.axis_size("gy")
    spans = goal_count * probe_count // TILE
    gram_spans = probe_count * probe_count // TILE
    f32 = jnp.float32
    hbm = pl.BlockSpec(memory_space=pltpu.HBM)
    smem = pl.BlockSpec(memory_space=pltpu.SMEM)
    vmem = pl.BlockSpec(memory_space=pltpu.VMEM)
    results = (
        jax.ShapeDtypeStruct((groups, nx, ny, LANES, nz), f32),
        jax.ShapeDtypeStruct((goal_count, probe_count), f32),
        jax.ShapeDtypeStruct((probe_count, probe_count), f32),
    )
    state, goal, gram = pl.pallas_call(
        whole_kernel,
        out_shape=tuple(pltpu.VMEM(r.shape, r.dtype) for r in results),
        in_specs=[hbm] * 7,
        out_specs=(vmem, vmem, vmem),
        scratch_shapes=[
            *[pltpu.VMEM((groups, nx + 2, ny + 2, LANES, nz), f32)] * 3,
            pltpu.VMEM((nx, ny // CHUNK, CHUNK, nz), f32),
            pltpu.VMEM((nx, ny // CHUNK, CHUNK, nz), f32),
            pltpu.VMEM((STEPS * SWEEPS, groups, ny // 2, LANES, nz), f32),
            pltpu.VMEM((devices, spans, TILE), f32),
            pltpu.VMEM((devices, spans, TILE), f32),
            pltpu.VMEM((gram_spans, TILE), f32),
            pltpu.VMEM((devices, gram_spans, TILE), f32),
            pltpu.SMEM((3,), f32),
            pltpu.SMEM((sensors,), jnp.int32),
            pltpu.SMEM((1,), jnp.int32),
            pltpu.VMEM((goal_count, sensors), f32),
            pltpu.VMEM((1, sensors), jnp.int32),
            pltpu.SemaphoreType.DMA((4, probe_count)),
            pltpu.SemaphoreType.DMA((5,)),
            pltpu.SemaphoreType.DMA((2, groups, 6)),
            pltpu.SemaphoreType.DMA((2, groups, 6)),
            pltpu.SemaphoreType.DMA((STEPS * SWEEPS, groups)),
            pltpu.SemaphoreType.DMA((STEPS * SWEEPS, groups)),
            pltpu.SemaphoreType.DMA((2, devices)),
            pltpu.SemaphoreType.DMA((2, devices)),
        ],
        compiler_params=pltpu.CompilerParams(
            collective_id=0, has_side_effects=True, vmem_limit_bytes=40 * 1024 * 1024
        ),
    )(
        pltpu.with_memory_space_constraint(wind_speed, pltpu.HBM),
        pltpu.with_memory_space_constraint(sensor_cell.reshape(sensors), pltpu.HBM),
        sensor_count.reshape(1),
        pltpu.with_memory_space_constraint(probes, pltpu.HBM),
        pltpu.with_memory_space_constraint(diffusivity.reshape(nx, ny // CHUNK, CHUNK, nz), pltpu.HBM),
        pltpu.with_memory_space_constraint(goal_weight.reshape(sensors, goal_count).T, pltpu.HBM),
        pltpu.with_memory_space_constraint(sensor_owner.reshape(1, sensors), pltpu.HBM),
    )
    return pl.pallas_call(
        store_kernel,
        out_shape=(jax.ShapeDtypeStruct(probes.shape, f32), *results[1:]),
        in_specs=[vmem] * 3,
        out_specs=(hbm, hbm, hbm),
        scratch_shapes=[pltpu.SemaphoreType.DMA((probe_count,)), pltpu.SemaphoreType.DMA((2,))],
        compiler_params=pltpu.CompilerParams(has_side_effects=True, vmem_limit_bytes=1024 * 1024),
    )(state, goal, gram)


def solution(mesh):
    placed = (
        P(None, "gx", "gy", None),
        P("gx", "gy", None),
        P(),
        P("gx", "gy", None),
        P("gx", "gy", None, None),
        P("gx", "gy"),
        P("gx", "gy", None, None),
    )
    return jax.shard_map(
        body,
        mesh=mesh,
        in_specs=placed,
        out_specs=(P(None, "gx", "gy", None), P(("gx", "gy"), None), P()),
        check_vma=False,
    )
```

```python
import math

import jax
import jax.numpy as jnp
from jax import lax
from jax.experimental import pallas as pl
from jax.experimental.pallas import tpu as pltpu
from jax.sharding import PartitionSpec as P

STEPS = 2
SWEEPS = 4

time_step = 2.0

LANES = 8
CHUNK = 8
DETOUR = 8
TILE = 128
MESH = pl.DeviceIdType.MESH


def buffers(k):
    read = 0 if k == 0 else 2 - k % 2
    written = 0 if k == SWEEPS - 1 else 1 + k % 2
    return read, 0, written


def chips_in_row(n_gx):
    row = math.isqrt(max(n_gx // 2, 0))
    return row if row >= 2 and 2 * row * row == n_gx else 0


def unflatten(flat, columns):
    per = TILE // columns
    sub = lax.broadcasted_iota(jnp.int32, (per, TILE), 0)
    lane = lax.broadcasted_iota(jnp.int32, (per, TILE), 1)
    tiles = []
    for t in range(flat.shape[0]):
        wide = jnp.broadcast_to(flat[t : t + 1], (per, TILE))
        rows = wide
        for j in range(1, per):
            rows = jnp.where(sub == j, pltpu.roll(wide, TILE - columns * j, 1), rows)
        tiles.append(jnp.where(lane < columns, rows, 0.0))
    return jnp.concatenate(tiles, axis=0)


def flatten(rows, columns):
    per = TILE // columns
    sub = lax.broadcasted_iota(jnp.int32, (per, TILE), 0)
    tiles = []
    for t in range(rows.shape[0] // per):
        part = rows[t * per : (t + 1) * per]
        flat = jnp.where(sub == 0, part, 0.0)
        for j in range(1, per):
            flat = flat + jnp.where(sub == j, pltpu.roll(part, columns * j, 1), 0.0)
        tiles.append(jnp.sum(flat, axis=0, keepdims=True))
    return jnp.concatenate(tiles, axis=0)


def whole_kernel(
    wind_in, cells_in, count_in, field, diffusivity, weights_in, owners_in,
    state, goal_out, gram_out,
    held0, held1, held2, inv, mix, passing, contrib, landed, gram_mine, gram_landed, wind, cells, count, weights, owners,
    load_sem, small_sem, send_sem, recv_sem, pass_recv, pass_send, term_sem, gram_sem,
):
    held = (held0, held1, held2)
    groups, nx, ny = held0.shape[0], held0.shape[1] - 2, held0.shape[2] - 2
    nz = held0.shape[4]
    tiles = nz // TILE
    part = passing.shape[3]
    pieces = (pl.ds(1, ny - 2 * part), pl.ds(1 + ny - 2 * part, part), pl.ds(1 + ny - part, part))
    gx, gy = lax.axis_index("gx"), lax.axis_index("gy")
    n_gx, n_gy = lax.axis_size("gx"), lax.axis_size("gy")
    devices = n_gx * n_gy
    me = gx * n_gy + gy
    xs, ys = pl.ds(1, nx), pl.ds(1, ny)
    row = chips_in_row(n_gx)

    def place(k):
        other = lax.rem(me + k, devices)
        return (lax.div(other, n_gy), lax.rem(other, n_gy))

    barrier = pltpu.get_barrier_semaphore()

    def greet(k, carry):
        pl.semaphore_signal(barrier, inc=1, device_id=place(k), device_id_type=MESH)
        return carry

    lax.fori_loop(1, devices, greet, 0)

    small = [
        pltpu.make_async_copy(src, dst, small_sem.at[i])
        for i, (src, dst) in enumerate(
            ((wind_in, wind), (cells_in, cells), (count_in, count), (weights_in, weights), (owners_in, owners))
        )
    ]
    small[0].start()

    def load(part, p):
        where = (pl.ds(0, 1), pl.ds(nx - 1, 1), pl.ds(1, nx - 2))[part]
        land = (pl.ds(1, 1), pl.ds(nx, 1), pl.ds(2, nx - 2))[part]
        return pltpu.make_async_copy(
            field.at[p, where],
            held0.at[p // LANES, land, ys, p % LANES],
            load_sem.at[part, p],
        )

    probes = groups * LANES
    for p in range(probes):
        load(0, p).start()
        load(1, p).start()
    for p in range(LANES):
        load(2, p).start()
    coefficient = pltpu.make_async_copy(diffusivity, mix, load_sem.at[3, 0])
    coefficient.start()
    for p in range(LANES, probes):
        load(2, p).start()
    for copy in small[1:]:
        copy.start()

    has_up, has_down = gx < n_gx - 1, gx > 0
    has_next, has_back = gy < n_gy - 1, gy > 0
    blank_x = jnp.zeros((ny, LANES, nz), jnp.float32)
    blank_y = jnp.zeros((nx, LANES, nz), jnp.float32)

    @pl.when(jnp.logical_not(has_down))
    def _():
        for b in range(3):
            for g in range(groups):
                held[b][g, 0, ys] = blank_x

    @pl.when(jnp.logical_not(has_up))
    def _():
        for b in range(3):
            for g in range(groups):
                held[b][g, nx + 1, ys] = blank_x

    @pl.when(jnp.logical_not(has_back))
    def _():
        for b in range(3):
            for g in range(groups):
                held[b][g, xs, 0] = blank_y

    @pl.when(jnp.logical_not(has_next))
    def _():
        for b in range(3):
            for g in range(groups):
                held[b][g, xs, ny + 1] = blank_y

    pl.semaphore_wait(barrier, devices - 1)

    if row:
        wide = 2 * row
        far_up = jnp.logical_and(has_up, lax.rem(gx, wide) == wide - 1)
        far_down = jnp.logical_and(has_down, lax.rem(gx, wide) == 0)
        passes = (
            jnp.logical_and(gx >= wide, lax.rem(gx, wide) == wide - 1),
            jnp.logical_and(gx < n_gx - wide, lax.rem(gx, wide) == 0),
        )
        pass_from = ((gx + wide, gy), (gx - wide, gy))
        pass_to = ((gx - wide + 1, gy), (gx + wide - 1, gy))
        near_up = jnp.logical_and(has_up, lax.rem(gx, wide) != wide - 1)
        near_down = jnp.logical_and(has_down, lax.rem(gx, wide) != 0)
    else:
        near_up, near_down = has_up, has_down

    routes = ((gx + 1, gy), (gx - 1, gy), (gx, gy + 1), (gx, gy - 1))
    sends = (has_up,) * 3 + (has_down,) * 3 + (has_next, has_back)
    receives = (has_down,) * 3 + (has_up,) * 3 + (has_back, has_next)
    UP, DOWN, SIDE = (1, 2, 0), (4, 5, 3), (6, 7)

    def face(d, b, g, turn):
        if d < 3:
            src, dst, target = held[b].at[g, nx, pieces[d]], held[b].at[g, 0, pieces[d]], routes[0]
        elif d < 6:
            src, dst, target = held[b].at[g, 1, pieces[d - 3]], held[b].at[g, nx + 1, pieces[d - 3]], routes[1]
        elif d == 6:
            src, dst, target = held[b].at[g, xs, ny], held[b].at[g, xs, 0], routes[2]
        else:
            src, dst, target = held[b].at[g, xs, 1], held[b].at[g, xs, ny + 1], routes[3]
        return pltpu.make_async_remote_copy(
            src_ref=src,
            dst_ref=dst,
            send_sem=send_sem.at[turn % 2, g, d],
            recv_sem=recv_sem.at[turn % 2, g, d],
            device_id=target,
            device_id_type=MESH,
        )

    def detour(way, c, b, g, turn):
        return pltpu.make_async_remote_copy(
            src_ref=held[b].at[g, (nx, 1)[way], pieces[c]],
            dst_ref=passing.at[turn, g, c - 1],
            send_sem=send_sem.at[turn % 2, g, 3 * way + c],
            recv_sem=pass_recv.at[turn, g, c - 1],
            device_id=pass_from[way],
            device_id_type=MESH,
        )

    def onward(way, c, b, g, turn):
        return pltpu.make_async_remote_copy(
            src_ref=passing.at[turn, g, c - 1],
            dst_ref=held[b].at[g, (0, nx + 1)[way], pieces[c]],
            send_sem=pass_send.at[turn, g, c - 1],
            recv_sem=recv_sem.at[turn % 2, g, 3 * way + c],
            device_id=pass_to[way],
            device_id_type=MESH,
        )

    def start(ways, b, g, turn):
        for d in ways:
            passed = row and d in (1, 2, 4, 5)
            @pl.when((near_up, near_down)[d // 3] if passed else sends[d])
            def _():
                face(d, b, g, turn).start()

            if passed:
                @pl.when((far_up, far_down)[d // 3])
                def _():
                    detour(d // 3, d % 3, b, g, turn).start()

    def wait_sends(b, g, turn):
        for d in range(8):
            @pl.when(sends[d])
            def _():
                face(d, b, g, turn).wait_send()

    def wait_recv(ways, b, g, turn):
        for d in ways:
            @pl.when(receives[d])
            def _():
                face(d, b, g, turn).wait_recv()

    def pass_on(b, g, turn):
        if row:
            for way in (0, 1):
                @pl.when(passes[way])
                def _():
                    for c in (1, 2):
                        detour(way, c, b, g, turn).wait_recv()
                        onward(way, c, b, g, turn).start()

    def pass_done(g, turn):
        if row:
            for way in (0, 1):
                @pl.when(passes[way])
                def _():
                    for c in (1, 2):
                        onward(way, c, 0, g, turn).wait_send()

    for g in range(groups):
        for p in range(g * LANES, (g + 1) * LANES):
            load(0, p).wait()
            load(1, p).wait()
        start(UP + DOWN, 0, g, 0)

    small[0].wait()
    w0, w1, w2 = time_step * wind[0], time_step * wind[1], time_step * wind[2]
    total_wind = wind[0] + wind[1] + wind[2]

    def coefficients(x, carry):
        a = mix[x]
        r = 1.0 / (1.0 + time_step * (6.0 * a + total_wind))
        inv[x] = jnp.where(a > 0.0, r, 0.0)
        mix[x] = jnp.where(a > 0.0, time_step * a * r, 0.0)
        return carry

    for g in range(groups):
        for p in range(g * LANES, (g + 1) * LANES):
            load(2, p).wait()
        start(SIDE, 0, g, 0)
        if g == 0:
            coefficient.wait()
            lax.fori_loop(0, nx, coefficients, 0)
    for g in range(groups):
        pass_on(0, g, 0)

    lane = lax.broadcasted_iota(jnp.int32, (LANES, TILE), 1)
    first, last_lane = lane == 0, lane == TILE - 1
    zero = jnp.zeros((LANES, TILE), jnp.float32)

    def plane(x, g, read, source, put, begin, end):
        def tile(b, x, y, t):
            return held[b][g, x, y, :, t * TILE : (t + 1) * TILE]

        low = [tile(read, x, begin - 1, t) for t in range(tiles)]
        centre = [tile(read, x, begin, t) for t in range(tiles)]
        for y in range(begin, end):
            i, k = divmod(y - 1, CHUNK)
            high = [tile(read, x, y + 1, t) for t in range(tiles)]
            down = [pltpu.roll(c, 1, 1) for c in centre]
            up = [pltpu.roll(c, TILE - 1, 1) for c in centre]
            for t in range(tiles):
                cols = slice(t * TILE, (t + 1) * TILE)
                z_low = lax.select(first, down[t - 1] if t else zero, down[t])
                z_high = lax.select(last_lane, up[t + 1] if t + 1 < tiles else zero, up[t])
                x_low = tile(read, x - 1, y, t)
                x_high = tile(read, x + 1, y, t)
                beside = (x_low + x_high) + (low[t] + high[t]) + (z_low + z_high)
                upwind = w0 * x_low + w1 * low[t] + w2 * z_low
                begun = tile(source, x, y, t)
                r = jnp.broadcast_to(inv[x - 1, i, k : k + 1, cols], (LANES, TILE))
                a = jnp.broadcast_to(mix[x - 1, i, k : k + 1, cols], (LANES, TILE))
                put(g, x, y, cols, (begun + upwind) * r + a * beside)
            low, centre = centre, high

    total = STEPS * SWEEPS

    def sweep(step, k, last=False):
        read, source, written = buffers(k)
        turn = step * SWEEPS + k
        if last:
            def put(g, x, y, cols, value):
                state[g, x - 1, y - 1, :, cols] = value
        else:
            def put(g, x, y, cols, value):
                held[written][g, x, y, :, cols] = value

        def group(g, carry):
            def end(i, carry):
                side = lax.rem(gx + i, 2)

                @pl.when(side == 1)
                def _():
                    wait_recv(DOWN, read, g, turn)

                @pl.when(side == 0)
                def _():
                    wait_recv(UP, read, g, turn)

                plane(1 + side * (nx - 1), g, read, source, put, 1, ny + 1)
                if not last:
                    @pl.when(side == 1)
                    def _():
                        start(UP, written, g, turn + 1)

                    @pl.when(side == 0)
                    def _():
                        start(DOWN, written, g, turn + 1)

                return carry

            def inner(x, carry):
                plane(x, g, read, source, put, 1, ny + 1)
                return carry

            @pl.when(turn >= 1)
            def _():
                wait_sends(read, g, turn - 1)

            wait_recv(SIDE, read, g, turn)
            if last:
                lax.fori_loop(2, nx, inner, 0)
            lax.fori_loop(0, 2, end, 0)
            if not last:
                lax.fori_loop(2, nx, inner, 0, unroll=2)
                start(SIDE, written, g, turn + 1)
                pass_on(written, g, turn + 1)
            return carry

        lax.fori_loop(0, groups, group, 0)

    def one_step(step, carry):
        for k in range(SWEEPS - 1):
            sweep(step, k)

        @pl.when(step < STEPS - 1)
        def _():
            sweep(step, SWEEPS - 1)

        return carry

    lax.fori_loop(0, STEPS, one_step, 0)
    sweep(STEPS - 1, SWEEPS - 1, True)
    for g in range(groups):
        wait_sends(0, g, total - 1)
        lax.fori_loop(0, total, lambda turn, carry: pass_done(g, turn) or carry, 0)
    for copy in small[1:]:
        copy.wait()

    sensors = cells.shape[0]

    column_of = lax.broadcasted_iota(jnp.int32, (LANES, nz), 1)
    unroll = math.gcd(sensors, 32)

    def look(i, carry):
        acc = list(carry)
        for k in range(unroll):
            s = i * unroll + k
            cell = cells[s]
            column = lax.div(cell, nz)
            hit = column_of == lax.rem(cell, nz)
            for g in range(groups):
                value = lax.select(hit, state[g, lax.div(column, ny), lax.rem(column, ny)], jnp.zeros((LANES, nz), jnp.float32))
                acc[g] = jnp.where(lane == s, jnp.sum(value, axis=1, keepdims=True), acc[g])
        return tuple(acc)

    readings = jnp.concatenate(lax.fori_loop(0, sensors // unroll, look, (zero,) * groups), axis=0)
    active = lax.broadcasted_iota(jnp.int32, (probes, sensors), 1) < count[0]
    readings = jnp.where(active, readings, 0.0)
    weight = weights[...]
    goal_count = weight.shape[0]
    outer = (weight[:, None, :] * readings[None, :, :]).reshape(goal_count * probes, sensors)
    onehot = (
        lax.broadcasted_iota(jnp.int32, (devices, sensors), 0) == jnp.broadcast_to(owners[...], (devices, sensors))
    ).astype(jnp.float32)
    terms = lax.dot_general(
        onehot, outer, (((1,), (1,)), ((), ())),
        precision=lax.Precision.HIGHEST, preferred_element_type=jnp.float32,
    )
    spans = contrib.shape[1]
    for t in range(spans):
        contrib[:, t, :] = terms[:, t * TILE : (t + 1) * TILE]

    def exchange(source, into, sem):
        def copy(k, slot):
            return pltpu.make_async_remote_copy(
                src_ref=source(k),
                dst_ref=into.at[slot],
                send_sem=sem.at[0, k],
                recv_sem=sem.at[1, k],
                device_id=place(k),
                device_id_type=MESH,
            )

        def send(k, carry):
            copy(k, me).start()
            return carry

        def finish(k, carry):
            arriving = copy(k, lax.rem(me + devices - k, devices))
            arriving.wait_send()
            arriving.wait_recv()
            return carry

        lax.fori_loop(1, devices, send, 0)
        into[pl.ds(me, 1)] = source(0)[...][None]
        lax.fori_loop(1, devices, finish, 0)
        return jnp.sum(into[...], axis=0)

    goal = exchange(lambda k: contrib.at[lax.rem(me + k, devices)], landed, term_sem)
    goal = unflatten(goal, probes)
    goal_out[...] = goal[:, :probes]
    gram = jnp.dot(
        goal.T[:probes], goal, precision=lax.Precision.HIGHEST, preferred_element_type=jnp.float32
    )
    gram_mine[...] = flatten(gram, probes)
    gram = exchange(lambda k: gram_mine, gram_landed, gram_sem)
    gram_out[...] = unflatten(gram, probes)[:, :probes]


def store_kernel(state, goal, gram, out, goal_out, gram_out, store_sem, small_sem):
    copies = [
        pltpu.make_async_copy(state.at[p // LANES, :, :, p % LANES], out.at[p], store_sem.at[p])
        for p in range(out.shape[0])
    ]
    copies.append(pltpu.make_async_copy(goal, goal_out, small_sem.at[0]))
    copies.append(pltpu.make_async_copy(gram, gram_out, small_sem.at[1]))
    for copy in copies:
        copy.start()
    for copy in copies:
        copy.wait()


def body(probes, diffusivity, wind_speed, sensor_cell, sensor_owner, sensor_count, goal_weight):
    probe_count, nx, ny, nz = probes.shape
    groups = probe_count // LANES
    sensors, goal_count = sensor_cell.shape[2], goal_weight.shape[3]
    devices = lax.axis_size("gx") * lax.axis_size("gy")
    spans = goal_count * probe_count // TILE
    gram_spans = probe_count * probe_count // TILE
    f32 = jnp.float32
    hbm = pl.BlockSpec(memory_space=pltpu.HBM)
    smem = pl.BlockSpec(memory_space=pltpu.SMEM)
    vmem = pl.BlockSpec(memory_space=pltpu.VMEM)
    results = (
        jax.ShapeDtypeStruct((groups, nx, ny, LANES, nz), f32),
        jax.ShapeDtypeStruct((goal_count, probe_count), f32),
        jax.ShapeDtypeStruct((probe_count, probe_count), f32),
    )
    state, goal, gram = pl.pallas_call(
        whole_kernel,
        out_shape=tuple(pltpu.VMEM(r.shape, r.dtype) for r in results),
        in_specs=[hbm] * 7,
        out_specs=(vmem, vmem, vmem),
        scratch_shapes=[
            *[pltpu.VMEM((groups, nx + 2, ny + 2, LANES, nz), f32)] * 3,
            pltpu.VMEM((nx, ny // CHUNK, CHUNK, nz), f32),
            pltpu.VMEM((nx, ny // CHUNK, CHUNK, nz), f32),
            pltpu.VMEM((STEPS * SWEEPS, groups, 2, ny * DETOUR // 32, LANES, nz), f32),
            pltpu.VMEM((devices, spans, TILE), f32),
            pltpu.VMEM((devices, spans, TILE), f32),
            pltpu.VMEM((gram_spans, TILE), f32),
            pltpu.VMEM((devices, gram_spans, TILE), f32),
            pltpu.SMEM((3,), f32),
            pltpu.SMEM((sensors,), jnp.int32),
            pltpu.SMEM((1,), jnp.int32),
            pltpu.VMEM((goal_count, sensors), f32),
            pltpu.VMEM((1, sensors), jnp.int32),
            pltpu.SemaphoreType.DMA((4, probe_count)),
            pltpu.SemaphoreType.DMA((5,)),
            pltpu.SemaphoreType.DMA((2, groups, 8)),
            pltpu.SemaphoreType.DMA((2, groups, 8)),
            pltpu.SemaphoreType.DMA((STEPS * SWEEPS, groups, 2)),
            pltpu.SemaphoreType.DMA((STEPS * SWEEPS, groups, 2)),
            pltpu.SemaphoreType.DMA((2, devices)),
            pltpu.SemaphoreType.DMA((2, devices)),
        ],
        compiler_params=pltpu.CompilerParams(
            collective_id=0, has_side_effects=True, vmem_limit_bytes=40 * 1024 * 1024
        ),
    )(
        pltpu.with_memory_space_constraint(wind_speed, pltpu.HBM),
        pltpu.with_memory_space_constraint(sensor_cell.reshape(sensors), pltpu.HBM),
        sensor_count.reshape(1),
        pltpu.with_memory_space_constraint(probes, pltpu.HBM),
        pltpu.with_memory_space_constraint(diffusivity.reshape(nx, ny // CHUNK, CHUNK, nz), pltpu.HBM),
        pltpu.with_memory_space_constraint(goal_weight.reshape(sensors, goal_count).T, pltpu.HBM),
        pltpu.with_memory_space_constraint(sensor_owner.reshape(1, sensors), pltpu.HBM),
    )
    return pl.pallas_call(
        store_kernel,
        out_shape=(jax.ShapeDtypeStruct(probes.shape, f32), *results[1:]),
        in_specs=[vmem] * 3,
        out_specs=(hbm, hbm, hbm),
        scratch_shapes=[pltpu.SemaphoreType.DMA((probe_count,)), pltpu.SemaphoreType.DMA((2,))],
        compiler_params=pltpu.CompilerParams(has_side_effects=True, vmem_limit_bytes=1024 * 1024),
    )(state, goal, gram)


def solution(mesh):
    placed = (
        P(None, "gx", "gy", None),
        P("gx", "gy", None),
        P(),
        P("gx", "gy", None),
        P("gx", "gy", None, None),
        P("gx", "gy"),
        P("gx", "gy", None, None),
    )
    return jax.shard_map(
        body,
        mesh=mesh,
        in_specs=placed,
        out_specs=(P(None, "gx", "gy", None), P(("gx", "gy"), None), P()),
        check_vma=False,
    )
```
